32 devices in a mesh: segment: 8 (over z, x), dp: 4 (over y, core).
Axes of the slice: x: 2, y: 2, z: 4, core: 2. Of those that a mesh axis runs over, the one named last changes fastest.
Arguments:
- src_embed: bfloat16 [16, 128, 2048], P('dp', None, 'segment'), parts along dimension 0, may hold values from -6 to 6
- tgt_embed: bfloat16 [16, 128, 2048], P('dp', None, 'segment'), parts along dimension 0, may hold values from -6 to 6
- src_lengths: int32 [16], P('dp'), parts along dimension 0, may hold values from 32 to 128
- tgt_lengths: int32 [16], P('dp'), parts along dimension 0, may hold values from 32 to 128
- attn_in: bfloat16 [8, 2048, 3072], P('segment'), may hold values from -0.125 to 0.125
- attn_out: bfloat16 [8, 1024, 2048], P('segment'), may hold values from -0.375 to 0.375
- norm_gain: float32 [4, 2048], replicated, may hold values from 0.25 to 1.75
- final_gain: float32 [2048], replicated, may hold values from 0.25 to 1.75
Outputs:
- decoded: bfloat16 [16, 128, 2048], P('dp', None, 'segment'), parts along dimension 0
The draws below stay inside these ranges and needn't reach their ends.
There are 4 independent parts, one for each index of `dp`. The reference program is written for one: setup_inputs(seed, part) draws one part's arguments, and reference() takes and returns one part's arrays. A program takes and returns all parts, laid end to end along the dimension named above; an argument that names none is the same for every part. Nothing has to cross between parts.
Inputs may be any that keep to these rules, and one draw needn't show every extreme that they name: `src_lengths`: keys at positions below a sequence's length are its real tokens. `tgt_lengths`: keys at positions below a sequence's length are its real tokens.
All inputs are finite; a program needn't handle non-finite values.
Results may differ from the reference program's by a relative error of at most 0.015.
Values may be sent and summed in bfloat16 or wider, within the bound.
A program may use at most 64 MiB of HBM per device.

```python
import jax
import jax.numpy as jnp
from jax import lax

D = 2048
HEAD = 64
MB = 4
S = 128
GROUP = 2
INNER = 2048
N_SEGMENT = 8


def place_ends(drawn, key, smallest, top_value):
    shape = drawn.shape
    index_at = [jax.random.randint(jax.random.fold_in(key, axis), (), 0, shape[axis]) for axis in range(len(shape))]
    drawn = drawn.at[tuple(index_at)].set(smallest)
    longest = shape.index(max(shape))
    index_at[longest] = (index_at[longest] + 1) % shape[longest]
    return drawn.at[tuple(index_at)].set(top_value)


def block_levels(stream_key, extent, cuts, low, top_value):
    def one(axis_at, blocks):
        steps = jax.random.uniform(jax.random.fold_in(jax.random.fold_in(stream_key, 6), axis_at), (blocks,), jnp.float32, low / len(cuts), top_value / len(cuts))
        return jnp.repeat(jnp.exp(steps), extent[axis_at] // blocks).reshape((-1,) + (1,) * (len(extent) - axis_at - 1))

    gain = one(*cuts[0])
    for cut in cuts[1:]:
        gain = gain * one(*cut)
    return gain


def centred(own_key, shape, deviation, most, cuts=(), kind=jnp.bfloat16):
    array = jax.random.normal(own_key, shape, jnp.float32) * deviation
    if len(cuts) > 0:
        array = block_levels(own_key, shape, cuts, -0.22, 0.18) * array
    return jnp.clip(array, min=-most, max=most).astype(kind)


def setup_inputs(seed: int = 0, part: int = 0) -> dict:
    key_list = jax.random.split(jax.random.key(seed), 9)
    part_keys = jax.random.split(jax.random.fold_in(key_list[8], part), 9)
    return {
        "src_embed": centred(part_keys[0], (MB, S, D), 1.0, 6.0, ((2, 8),)),
        "tgt_embed": centred(part_keys[1], (MB, S, D), 1.0, 6.0, ((2, 8),)),
        "src_lengths": place_ends(jax.random.randint(part_keys[2], (MB,), S // 4, S + 1), jax.random.fold_in(part_keys[2], 1), S // 4, S).astype(jnp.int32),
        "tgt_lengths": place_ends(jax.random.randint(part_keys[3], (MB,), S // 4, S + 1), jax.random.fold_in(part_keys[3], 1), S // 4, S).astype(jnp.int32),
        "attn_in": centred(key_list[4], (N_SEGMENT, D, 3 * INNER // GROUP), D ** -0.5, 0.125, ((0, 8),)),
        "attn_out": centred(key_list[5], (N_SEGMENT, INNER // GROUP, D), (INNER // 8) ** -0.5, 0.375, ((0, 8),)),
        "norm_gain": jnp.clip(1.0 + 0.15 * jax.random.normal(key_list[6], (4, D), jnp.float32), 0.25, 1.75),
        "final_gain": jnp.clip(1.0 + 0.15 * jax.random.normal(key_list[7], (D,), jnp.float32), 0.25, 1.75),
    }


epsilon = 1e-06
score_scale = 0.125

def rms_scale(values, gain_vector):
    return values * lax.rsqrt(lax.optimization_barrier(jnp.mean(values * values, axis=-1, keepdims=True)) + epsilon) * gain_vector

def attention(queries, key_rows, values, allowed):
    head_count = queries.shape[1] // HEAD
    shaped_q = queries.reshape(queries.shape[0], head_count, HEAD).astype(jnp.float32)
    shaped_k = key_rows.reshape(key_rows.shape[0], head_count, HEAD).astype(jnp.float32)
    shaped_v = values.reshape(values.shape[0], head_count, HEAD).astype(jnp.float32)
    scores = jnp.einsum('qhd,khd->hqk', shaped_q, shaped_k) * score_scale
    scores = jnp.where(allowed[None], scores, -1000000000.0)
    weights = jax.nn.softmax(scores, axis=-1).astype(jnp.bfloat16)
    mixture = jnp.einsum('hqk,khd->qhd', weights.astype(jnp.float32), shaped_v)
    return mixture.reshape(queries.shape[0], -1).astype(jnp.bfloat16)

def sublayer(inputs, memory, attn_in, attn_out, norm_gain, layer_slot, group_size, allowed):
    normed = rms_scale(inputs.astype(jnp.float32), norm_gain[layer_slot]).astype(jnp.bfloat16)
    source = normed if memory is None else memory
    summed = jnp.zeros(inputs.shape, jnp.float32)
    for member in range(group_size):
        weight_slot = layer_slot * group_size + member
        in_weight = attn_in[weight_slot]
        out_weight = attn_out[weight_slot]
        head_cols = out_weight.shape[0]
        queries = jnp.dot(normed, in_weight[:, :head_cols], preferred_element_type=jnp.float32).astype(jnp.bfloat16)
        key_value = jnp.dot(source, in_weight[:, head_cols:], preferred_element_type=jnp.float32).astype(jnp.bfloat16)
        mixture = attention(queries, key_value[:, :head_cols], key_value[:, head_cols:], allowed)
        summed = summed + jnp.dot(mixture, out_weight, preferred_element_type=jnp.float32)
    return (inputs.astype(jnp.float32) + summed).astype(jnp.bfloat16)

def reference(src_embed, tgt_embed, src_lengths, tgt_lengths, attn_in, attn_out, norm_gain, final_gain):
    group_size = N_SEGMENT // 4
    positions = jnp.arange(S, dtype=jnp.int32)
    causal = positions[None, :] <= positions[:, None]
    results = []
    for batch_slot in range(MB):
        source_ok = jnp.broadcast_to(positions[None, :] < src_lengths[batch_slot], (S, S))
        target_ok = (positions[None, :] < tgt_lengths[batch_slot]) & causal
        encoded = src_embed[batch_slot]
        for layer_slot in range(2):
            encoded = sublayer(encoded, None, attn_in, attn_out, norm_gain, layer_slot, group_size, source_ok)
        memory = rms_scale(encoded.astype(jnp.float32), final_gain).astype(jnp.bfloat16)
        decoded = sublayer(tgt_embed[batch_slot], memory, attn_in, attn_out, norm_gain, 2, group_size, source_ok)
        decoded = sublayer(decoded, None, attn_in, attn_out, norm_gain, 3, group_size, target_ok)
        results.append(decoded)
    return jnp.stack(results)
```

```python
import functools

import jax
import jax.numpy as jnp
from jax import lax
from jax.experimental import pallas as pl
from jax.experimental.pallas import tpu as pltpu
from jax.sharding import PartitionSpec as P

HEAD = 64
LAYERS = 4
MESH = pl.DeviceIdType.MESH
epsilon = 1e-06
score_scale = 0.125


def kernel(
    segs,
    src_len,
    tgt_len,
    src,
    tgt,
    w_in,
    w_out,
    gains,
    final_gain,
    out,
    win,
    wout,
    act,
    nrm,
    qkv,
    mix,
    own,
    ps,
    pr,
    fw,
    w_sem,
    act_sem,
    in_send,
    p_send,
    p_recv,
    f_send,
    o_recv,
):
    group = segs // LAYERS
    batches, seq, cw = src.shape
    width = segs * cw
    hc = wout.shape[0]
    me = lax.axis_index("segment")
    section = me // group
    member = me % group
    is_cross = section == 2
    is_last = section == LAYERS - 1
    q_src = jnp.where(is_cross, 1, 0)

    win_copy = pltpu.make_async_copy(w_in, win, w_sem.at[0])
    wout_copy = pltpu.make_async_copy(w_out, wout, w_sem.at[1])
    win_copy.start()
    wout_copy.start()

    barrier = pltpu.get_barrier_semaphore()
    for step in range(1, segs):
        pl.semaphore_signal(
            barrier,
            inc=1,
            device_id={"segment": lax.rem(me + step, segs)},
            device_id_type=MESH,
        )
    pl.semaphore_wait(barrier, segs - 1)

    def remote(source, dest, send, recv, target):
        return pltpu.make_async_remote_copy(
            src_ref=source,
            dst_ref=dest,
            send_sem=send,
            recv_sem=recv,
            device_id={"segment": target},
            device_id_type=MESH,
        )

    def input_copy(kind, m, j):
        ref = src if kind == 0 else tgt
        target = 2 * kind * group + j
        return remote(
            ref.at[m],
            act.at[kind, m, me],
            in_send.at[kind, m, j],
            act_sem.at[kind, m, me],
            target,
        )

    def send_inputs(kind, m):
        ref = src if kind == 0 else tgt
        for j in range(group):
            target = 2 * kind * group + j

            @pl.when(me != target)
            def _():
                input_copy(kind, m, j).start()

            @pl.when(me == target)
            def _():
                pltpu.make_async_copy(
                    ref.at[m], act.at[kind, m, me], act_sem.at[kind, m, me]
                ).start()

    for m in range(batches):
        send_inputs(0, m)
    for m in range(batches):
        send_inputs(1, m)

    def act_wait(kind, m, c):
        pltpu.make_async_copy(
            act.at[kind, m, c], act.at[kind, m, c], act_sem.at[kind, m, c]
        ).wait()

    def normalize(kind, m, gain_row):
        total = jnp.zeros((seq, cw), jnp.float32)
        for c in range(segs):
            v = act[kind, m, c].astype(jnp.float32)
            total = total + v * v
        mean = jnp.sum(total, axis=-1, keepdims=True) * (1.0 / width)
        scale = lax.rsqrt(mean + epsilon)
        for c in range(segs):
            v = act[kind, m, c].astype(jnp.float32)
            g = gain_row(c)
            nrm[kind, :, c * cw : (c + 1) * cw] = (v * scale * g).astype(jnp.bfloat16)

    def key_gain(c):
        cols = slice(c * cw, (c + 1) * cw)
        picked = jnp.where(is_cross, final_gain[:, cols], gains[0:1, cols])
        for p in (1, 3):
            picked = jnp.where(section == p, gains[p : p + 1, cols], picked)
        return picked

    def query_gain(c):
        return gains[2:3, c * cw : (c + 1) * cw]

    def part_copy(m, c, g):
        target = section * group + lax.rem(member + g, group)
        return remote(
            ps.at[m, c],
            pr.at[m, g - 1, c],
            p_send.at[m, g - 1, c],
            p_recv.at[m, g - 1, c],
            target,
        )

    def part_needed(c, g):
        goal = lax.rem(member + g, group)
        return jnp.logical_or(section < LAYERS - 1, lax.rem(c, group) == goal)

    def keeps(c):
        return jnp.logical_or(section < LAYERS - 1, lax.rem(c, group) == member)

    def next_copy(m, c):
        return remote(
            fw.at[m, c], act.at[0, m, c], f_send.at[m, c], act_sem.at[0, m, c], me + group
        )

    def out_copy(m, c):
        return remote(fw.at[m, c], out.at[m], f_send.at[m, c], o_recv.at[m], c)

    tile = min(512, hc)
    kv_tiles = 2 * hc // tile
    q_tiles = hc // tile

    def batch_step(m, carry):
        @pl.when(is_cross)
        def _():
            for c in range(segs):
                act_wait(1, m, c)
            normalize(1, m, query_gain)

        for c in range(segs):
            act_wait(0, m, c)

        normalize(0, m, key_gain)

        @pl.when(m == 0)
        def _():
            win_copy.wait()

        def project(t, carry):
            kind = jnp.where(t < q_tiles, q_src, 0)
            cols = pl.ds(pl.multiple_of(t * tile, tile), tile)
            qkv[:, cols] = jnp.dot(
                nrm[kind], win[:, cols], preferred_element_type=jnp.float32
            ).astype(jnp.bfloat16)
            return carry

        lax.fori_loop(0, q_tiles + kv_tiles, project, 0)

        length = jnp.where(is_last, tgt_len[m], src_len[m])
        keys = lax.broadcasted_iota(jnp.int32, (2 * seq, seq), 1)
        rows = lax.broadcasted_iota(jnp.int32, (2 * seq, seq), 0)
        rows = jnp.where(rows >= seq, rows - seq, rows)
        bound = jnp.where(is_last, rows, seq)
        allowed = (keys < length) & (keys <= bound)
        lane = lax.broadcasted_iota(jnp.int32, (seq, 2 * HEAD), 1)
        low = lane < HEAD
        for h in range(hc // (2 * HEAD)):
            at = h * 2 * HEAD
            q2 = qkv[:, at : at + 2 * HEAD]
            k2 = qkv[:, hc + at : hc + at + 2 * HEAD]
            v2 = qkv[:, 2 * hc + at : 2 * hc + at + 2 * HEAD]
            zero = jnp.zeros_like(q2)
            both = jnp.concatenate(
                [jnp.where(low, q2, zero), jnp.where(low, zero, q2)], axis=0
            )
            scores = (
                lax.dot_general(
                    both,
                    k2,
                    (((1,), (1,)), ((), ())),
                    preferred_element_type=jnp.float32,
                )
                * score_scale
            )
            scores = jnp.where(allowed, scores, -1000000000.0)
            top = jnp.max(scores, axis=-1, keepdims=True)
            e = jnp.exp(scores - top)
            weights = (e / jnp.sum(e, axis=-1, keepdims=True)).astype(jnp.bfloat16)
            o = jnp.dot(weights, v2, preferred_element_type=jnp.float32)
            mix[:, at : at + 2 * HEAD] = jnp.where(low, o[:seq], o[seq:]).astype(
                jnp.bfloat16
            )

        @pl.when(m == 0)
        def _():
            wout_copy.wait()

        def emit(c, carry):
            cols = pl.ds(pl.multiple_of(c * cw, cw), cw)
            part = jnp.dot(mix[...], wout[:, cols], preferred_element_type=jnp.float32)
            own[c] = part
            ps[m, c] = part.astype(jnp.bfloat16)
            for g in range(1, group):

                @pl.when(part_needed(c, g))
                def _():
                    part_copy(m, c, g).start()

            return carry

        lax.fori_loop(0, segs, emit, 0)

        def combine(c, carry):
            @pl.when(keeps(c))
            def _():
                total = own[c] + act[q_src, m, c].astype(jnp.float32)
                for g in range(1, group):
                    part_copy(m, c, g).wait_recv()
                    total = total + pr[m, g - 1, c].astype(jnp.float32)
                fw[m, c] = total.astype(jnp.bfloat16)

                @pl.when(section < LAYERS - 1)
                def _():
                    next_copy(m, c).start()

                @pl.when(jnp.logical_and(is_last, me != c))
                def _():
                    out_copy(m, c).start()

                @pl.when(jnp.logical_and(is_last, me == c))
                def _():
                    pltpu.make_async_copy(fw.at[m, c], out.at[m], o_recv.at[m]).start()

            return carry

        lax.fori_loop(0, segs, combine, 0)
        return carry

    lax.fori_loop(0, batches, batch_step, 0)

    def finish(m, carry):
        for kind in range(2):
            for j in range(group):

                @pl.when(me != 2 * kind * group + j)
                def _():
                    input_copy(kind, m, j).wait_send()

        def drain(c, carry):
            for g in range(1, group):

                @pl.when(part_needed(c, g))
                def _():
                    part_copy(m, c, g).wait_send()

            @pl.when(section < LAYERS - 1)
            def _():
                next_copy(m, c).wait_send()

            @pl.when(jnp.logical_and(is_last, jnp.logical_and(keeps(c), me != c)))
            def _():
                out_copy(m, c).wait_send()

            return carry

        lax.fori_loop(0, segs, drain, 0)
        pltpu.make_async_copy(out.at[m], out.at[m], o_recv.at[m]).wait()
        return carry

    lax.fori_loop(0, batches, finish, 0)


def solution(mesh):
    segs = mesh.shape["segment"]

    def on_device(src, tgt, src_len, tgt_len, w_in, w_out, gains, final_gain):
        batches, seq, cw = src.shape
        group = segs // LAYERS
        w_in, w_out = w_in[0], w_out[0]
        width, qkv_cols = w_in.shape
        hc = w_out.shape[0]
        vmem = pl.BlockSpec(memory_space=pltpu.VMEM)
        smem = pl.BlockSpec(memory_space=pltpu.SMEM)
        anym = pl.BlockSpec(memory_space=pl.ANY)
        bf16 = jnp.bfloat16
        block = (segs, seq, cw)
        dma = pltpu.SemaphoreType.DMA
        return pl.pallas_call(
            functools.partial(kernel, segs),
            out_shape=jax.ShapeDtypeStruct(src.shape, src.dtype),
            in_specs=[smem, smem, vmem, vmem, anym, anym, vmem, vmem],
            out_specs=vmem,
            scratch_shapes=[
                pltpu.VMEM((width, qkv_cols), bf16),
                pltpu.VMEM((hc, width), bf16),
                pltpu.VMEM((2, batches) + block, bf16),
                pltpu.VMEM((2, seq, width), bf16),
                pltpu.VMEM((seq, qkv_cols), bf16),
                pltpu.VMEM((seq, hc), bf16),
                pltpu.VMEM(block, jnp.float32),
                pltpu.VMEM((batches,) + block, bf16),
                pltpu.VMEM((batches, group - 1) + block, bf16),
                pltpu.VMEM((batches,) + block, bf16),
                dma((2,)),
                dma((2, batches, segs)),
                dma((2, batches, group)),
                dma((batches, group - 1, segs)),
                dma((batches, group - 1, segs)),
                dma((batches, segs)),
                dma((batches,)),
            ],
            compiler_params=pltpu.CompilerParams(
                collective_id=0,
                has_side_effects=True,
                vmem_limit_bytes=56 * 1024 * 1024,
            ),
        )(src_len, tgt_len, src, tgt, w_in, w_out, gains, final_gain[None])

    return jax.shard_map(
        on_device,
        mesh=mesh,
        in_specs=(
            P("dp", None, "segment"),
            P("dp", None, "segment"),
            P("dp"),
            P("dp"),
            P("segment", None, None),
            P("segment", None, None),
            P(),
            P(),
        ),
        out_specs=P("dp", None, "segment"),
        check_vma=False,
    )
```

```python
import functools

import jax
import jax.numpy as jnp
from jax import lax
from jax.experimental import pallas as pl
from jax.experimental.pallas import tpu as pltpu
from jax.sharding import PartitionSpec as P

HEAD = 64
LAYERS = 4
MESH = pl.DeviceIdType.MESH
epsilon = 1e-06
score_scale = 0.125


def kernel(
    segs,
    src_len,
    tgt_len,
    src,
    tgt,
    w_in,
    w_out,
    gains,
    final_gain,
    out,
    win,
    wout,
    act,
    nrm,
    qkv,
    mix,
    own,
    ps,
    pr,
    fw,
    w_sem,
    act_sem,
    in_send,
    p_send,
    p_recv,
    f_send,
    o_recv,
    go,
    side,
    side_send,
    side_recv,
    on_send,
    r_send,
):
    group = segs // LAYERS
    batches, seq, cw = src.shape
    width = segs * cw
    hc = wout.shape[0]
    me = lax.axis_index("segment")
    section = me // group
    member = me % group
    is_cross = section == 2
    is_last = section == LAYERS - 1
    q_src = jnp.where(is_cross, 1, 0)

    win_copy = pltpu.make_async_copy(w_in, win, w_sem.at[0])
    wout_copy = pltpu.make_async_copy(w_out, wout, w_sem.at[1])
    win_copy.start()
    wout_copy.start()

    barrier = pltpu.get_barrier_semaphore()
    for step in range(1, segs):
        pl.semaphore_signal(
            barrier,
            inc=1,
            device_id={"segment": lax.rem(me + step, segs)},
            device_id_type=MESH,
        )
    pl.semaphore_wait(barrier, segs - 1)

    def remote(source, dest, send, recv, target):
        return pltpu.make_async_remote_copy(
            src_ref=source,
            dst_ref=dest,
            send_sem=send,
            recv_sem=recv,
            device_id={"segment": target},
            device_id_type=MESH,
        )

    def input_copy(kind, m, j):
        ref = src if kind == 0 else tgt
        target = 2 * kind * group + j
        return remote(
            ref.at[m],
            act.at[kind, m, me],
            in_send.at[kind, m, j],
            act_sem.at[kind, m, me],
            target,
        )

    def sends(kind, m, j):
        if kind == 1:
            return jnp.bool_(True)
        return jnp.logical_or(j == member, jnp.logical_and(section == 0, m > 0))

    def send_inputs(kind, m):
        ref = src if kind == 0 else tgt
        for j in range(group):
            target = 2 * kind * group + j

            @pl.when(jnp.logical_and(sends(kind, m, j), me != target))
            def _():
                input_copy(kind, m, j).start()

            @pl.when(me == target)
            def _():
                pltpu.make_async_copy(
                    ref.at[m], act.at[kind, m, me], act_sem.at[kind, m, me]
                ).start()

    def beside(g):
        return section * group + lax.rem(member + g, group)

    def side_copy(m, g):
        return remote(
            src.at[m],
            side.at[m - 1, g - 1],
            side_send.at[m - 1, g - 1],
            side_recv.at[m - 1, g - 1],
            beside(g),
        )

    def side_on(m, g):
        source = beside(group - g)
        return remote(
            side.at[m - 1, g - 1],
            act.at[0, m, source],
            on_send.at[m - 1, g - 1],
            act_sem.at[0, m, source],
            member,
        )

    def relay(c, g):
        return remote(
            act.at[0, 0, c],
            act.at[0, 0, c],
            r_send.at[g - 1, c],
            act_sem.at[0, 0, c],
            beside(g),
        )

    send_inputs(0, 0)

    @pl.when(section > 0)
    def _():
        for m in range(1, batches):
            for g in range(1, group):
                side_copy(m, g).start()

    @pl.when(section <= 2)
    def _():
        for m in range(batches):
            send_inputs(1, m)

    def act_wait(kind, m, c):
        pltpu.make_async_copy(
            act.at[kind, m, c], act.at[kind, m, c], act_sem.at[kind, m, c]
        ).wait()

    def pass_on():
        for c in range(segs):

            @pl.when(c % group == member)
            def _(c=c):
                act_wait(0, 0, c)
                for g in range(1, group):
                    relay(c, g).start()

    @pl.when(section == 0)
    def _():
        pass_on()
        for step in range(1, segs):
            pl.semaphore_signal(
                go,
                inc=1,
                device_id={"segment": lax.rem(me + step, segs)},
                device_id_type=MESH,
            )

    pl.semaphore_wait(go, jnp.where(section == 0, group - 1, group))
    for m in range(1, batches):
        send_inputs(0, m)

        @pl.when(section > 0)
        def _(m=m):
            for g in range(1, group):
                side_copy(m, g).wait_recv()
                side_on(m, g).start()

    @pl.when(section > 2)
    def _():
        for m in range(batches):
            send_inputs(1, m)

    def normalize(kind, m, gain_row):
        total = jnp.zeros((seq, cw), jnp.float32)
        for c in range(segs):
            v = act[kind, m, c].astype(jnp.float32)
            total = total + v * v
        mean = jnp.sum(total, axis=-1, keepdims=True) * (1.0 / width)
        scale = lax.rsqrt(mean + epsilon)
        for c in range(segs):
            v = act[kind, m, c].astype(jnp.float32)
            g = gain_row(c)
            nrm[kind, :, c * cw : (c + 1) * cw] = (v * scale * g).astype(jnp.bfloat16)

    def key_gain(c):
        cols = slice(c * cw, (c + 1) * cw)
        picked = jnp.where(is_cross, final_gain[:, cols], gains[0:1, cols])
        for p in (1, 3):
            picked = jnp.where(section == p, gains[p : p + 1, cols], picked)
        return picked

    def query_gain(c):
        return gains[2:3, c * cw : (c + 1) * cw]

    def part_copy(m, c, g):
        target = section * group + lax.rem(member + g, group)
        return remote(
            ps.at[m, c],
            pr.at[m, g - 1, c],
            p_send.at[m, g - 1, c],
            p_recv.at[m, g - 1, c],
            target,
        )

    def whole(m):
        return jnp.logical_and(section < LAYERS - 1, m > 0)

    def part_needed(m, c, g):
        goal = lax.rem(member + g, group)
        return jnp.logical_or(whole(m), lax.rem(c, group) == goal)

    def keeps(m, c):
        return jnp.logical_or(whole(m), lax.rem(c, group) == member)

    def next_copy(m, c):
        return remote(
            fw.at[m, c], act.at[0, m, c], f_send.at[m, c], act_sem.at[0, m, c], me + group
        )

    def out_copy(m, c):
        return remote(fw.at[m, c], out.at[m], f_send.at[m, c], o_recv.at[m], c)

    tile = min(512, hc)
    kv_tiles = 2 * hc // tile
    q_tiles = hc // tile

    def prepare(m):
        @pl.when(is_cross)
        def _():
            for c in range(segs):
                act_wait(1, m, c)
            normalize(1, m, query_gain)

        @pl.when(jnp.logical_and(section > 0, m == 0))
        def _():
            pass_on()

        for c in range(segs):

            @pl.when(jnp.logical_or(m > 0, c % group != member))
            def _(c=c):
                act_wait(0, m, c)

        normalize(0, m, key_gain)

        @pl.when(m == 0)
        def _():
            win_copy.wait()


    def project(t, carry):
        kind = jnp.where(t < q_tiles, q_src, 0)
        cols = pl.ds(pl.multiple_of(t * tile, tile), tile)
        qkv[:, cols] = jnp.dot(
            nrm[kind], win[:, cols], preferred_element_type=jnp.float32
        ).astype(jnp.bfloat16)
        return carry

    def attend(m):
        length = jnp.where(is_last, tgt_len[m], src_len[m])
        keys = lax.broadcasted_iota(jnp.int32, (2 * seq, seq), 1)
        rows = lax.broadcasted_iota(jnp.int32, (2 * seq, seq), 0)
        rows = jnp.where(rows >= seq, rows - seq, rows)
        bound = jnp.where(is_last, rows, seq)
        allowed = (keys < length) & (keys <= bound)
        lane = lax.broadcasted_iota(jnp.int32, (seq, 2 * HEAD), 1)
        low = lane < HEAD
        for h in range(hc // (2 * HEAD)):
            at = h * 2 * HEAD
            q2 = qkv[:, at : at + 2 * HEAD]
            k2 = qkv[:, hc + at : hc + at + 2 * HEAD]
            v2 = qkv[:, 2 * hc + at : 2 * hc + at + 2 * HEAD]
            zero = jnp.zeros_like(q2)
            both = jnp.concatenate(
                [jnp.where(low, q2, zero), jnp.where(low, zero, q2)], axis=0
            )
            scores = (
                lax.dot_general(
                    both,
                    k2,
                    (((1,), (1,)), ((), ())),
                    preferred_element_type=jnp.float32,
                )
                * score_scale
            )
            scores = jnp.where(allowed, scores, -1000000000.0)
            top = jnp.max(scores, axis=-1, keepdims=True)
            e = jnp.exp(scores - top)
            weights = (e / jnp.sum(e, axis=-1, keepdims=True)).astype(jnp.bfloat16)
            o = jnp.dot(weights, v2, preferred_element_type=jnp.float32)
            mix[:, at : at + 2 * HEAD] = jnp.where(low, o[:seq], o[seq:]).astype(
                jnp.bfloat16
            )

    def send_parts(m):
        @pl.when(m == 0)
        def _():
            wout_copy.wait()

        def emit(c, carry):
            cols = pl.ds(pl.multiple_of(c * cw, cw), cw)
            part = jnp.dot(mix[...], wout[:, cols], preferred_element_type=jnp.float32)
            own[c] = part
            ps[m, c] = part.astype(jnp.bfloat16)
            for g in range(1, group):

                @pl.when(part_needed(m, c, g))
                def _():
                    part_copy(m, c, g).start()

            return carry

        lax.fori_loop(0, segs, emit, 0)

    def combine(m, c):
        @pl.when(keeps(m, c))
        def _():
            total = own[c] + act[q_src, m, c].astype(jnp.float32)
            for g in range(1, group):
                part_copy(m, c, g).wait_recv()
                total = total + pr[m, g - 1, c].astype(jnp.float32)
            fw[m, c] = total.astype(jnp.bfloat16)

            @pl.when(section < LAYERS - 1)
            def _():
                next_copy(m, c).start()

            @pl.when(jnp.logical_and(is_last, me != c))
            def _():
                out_copy(m, c).start()

            @pl.when(jnp.logical_and(is_last, me == c))
            def _():
                pltpu.make_async_copy(fw.at[m, c], out.at[m], o_recv.at[m]).start()

    half = (q_tiles + kv_tiles) // 2
    stages = (
        prepare,
        lambda m: lax.fori_loop(0, half, project, 0),
        lambda m: lax.fori_loop(half, q_tiles + kv_tiles, project, 0),
        attend,
    )

    def batch_step(t, carry):
        m = t - 1

        @pl.when(t > 0)
        def _():
            send_parts(m)

        for c in range(segs):
            for i, stage in enumerate(stages):
                if c == segs // 2 + i * segs // 8:

                    @pl.when(t < batches)
                    def _(stage=stage):
                        stage(t)

            @pl.when(t > 0)
            def _(c=c):
                combine(m, c)

        return carry

    lax.fori_loop(0, batches + 1, batch_step, 0)

    def finish(m, carry):
        for kind in range(2):
            for j in range(group):

                @pl.when(jnp.logical_and(sends(kind, m, j), me != 2 * kind * group + j))
                def _():
                    input_copy(kind, m, j).wait_send()

        @pl.when(jnp.logical_and(section > 0, m > 0))
        def _():
            for g in range(1, group):
                side_copy(m, g).wait_send()
                side_on(m, g).wait_send()

        def drain(c, carry):
            for g in range(1, group):

                @pl.when(part_needed(m, c, g))
                def _():
                    part_copy(m, c, g).wait_send()

            @pl.when(jnp.logical_and(section < LAYERS - 1, keeps(m, c)))
            def _():
                next_copy(m, c).wait_send()

            @pl.when(jnp.logical_and(m == 0, lax.rem(c, group) == member))
            def _():
                for g in range(1, group):
                    relay(c, g).wait_send()

            @pl.when(jnp.logical_and(is_last, jnp.logical_and(keeps(m, c), me != c)))
            def _():
                out_copy(m, c).wait_send()

            return carry

        lax.fori_loop(0, segs, drain, 0)
        pltpu.make_async_copy(out.at[m], out.at[m], o_recv.at[m]).wait()
        return carry

    lax.fori_loop(0, batches, finish, 0)


def solution(mesh):
    segs = mesh.shape["segment"]

    def on_device(src, tgt, src_len, tgt_len, w_in, w_out, gains, final_gain):
        batches, seq, cw = src.shape
        group = segs // LAYERS
        w_in, w_out = w_in[0], w_out[0]
        width, qkv_cols = w_in.shape
        hc = w_out.shape[0]
        vmem = pl.BlockSpec(memory_space=pltpu.VMEM)
        smem = pl.BlockSpec(memory_space=pltpu.SMEM)
        anym = pl.BlockSpec(memory_space=pl.ANY)
        bf16 = jnp.bfloat16
        block = (segs, seq, cw)
        dma = pltpu.SemaphoreType.DMA
        return pl.pallas_call(
            functools.partial(kernel, segs),
            out_shape=jax.ShapeDtypeStruct(src.shape, src.dtype),
            in_specs=[smem, smem, vmem, vmem, anym, anym, vmem, vmem],
            out_specs=vmem,
            scratch_shapes=[
                pltpu.VMEM((width, qkv_cols), bf16),
                pltpu.VMEM((hc, width), bf16),
                pltpu.VMEM((2, batches) + block, bf16),
                pltpu.VMEM((2, seq, width), bf16),
                pltpu.VMEM((seq, qkv_cols), bf16),
                pltpu.VMEM((seq, hc), bf16),
                pltpu.VMEM(block, jnp.float32),
                pltpu.VMEM((batches,) + block, bf16),
                pltpu.VMEM((batches, group - 1) + block, bf16),
                pltpu.VMEM((batches,) + block, bf16),
                dma((2,)),
                dma((2, batches, segs)),
                dma((2, batches, group)),
                dma((batches, group - 1, segs)),
                dma((batches, group - 1, segs)),
                dma((batches, segs)),
                dma((batches,)),
                pltpu.SemaphoreType.REGULAR,
                pltpu.VMEM((batches - 1, group - 1, seq, cw), bf16),
                dma((batches - 1, group - 1)),
                dma((batches - 1, group - 1)),
                dma((batches - 1, group - 1)),
                dma((group - 1, segs)),
            ],
            compiler_params=pltpu.CompilerParams(
                collective_id=0,
                has_side_effects=True,
                vmem_limit_bytes=56 * 1024 * 1024,
            ),
        )(src_len, tgt_len, src, tgt, w_in, w_out, gains, final_gain[None])

    return jax.shard_map(
        on_device,
        mesh=mesh,
        in_specs=(
            P("dp", None, "segment"),
            P("dp", None, "segment"),
            P("dp"),
            P("dp"),
            P("segment", None, None),
            P("segment", None, None),
            P(),
            P(),
        ),
        out_specs=P("dp", None, "segment"),
        check_vma=False,
    )
```

```python
import functools

import jax
import jax.numpy as jnp
from jax import lax
from jax.experimental import pallas as pl
from jax.experimental.pallas import tpu as pltpu
from jax.sharding import PartitionSpec as P

HEAD = 64
LAYERS = 4
MESH = pl.DeviceIdType.MESH
epsilon = 1e-06
score_scale = 0.125


def kernel(
    segs,
    src_len,
    tgt_len,
    src,
    tgt,
    w_in,
    w_out,
    gains,
    final_gain,
    out,
    win,
    wout,
    act,
    nrm,
    qkv,
    mix,
    own,
    ps,
    pr,
    fw,
    w_sem,
    act_sem,
    in_send,
    p_send,
    p_recv,
    f_send,
    o_recv,
    go,
    side,
    side_send,
    side_recv,
    on_send,
    r_send,
):
    group = segs // LAYERS
    batches, seq, cw = src.shape
    width = segs * cw
    hc = wout.shape[0]
    me = lax.axis_index("segment")
    section = me // group
    member = me % group
    is_cross = section == 2
    is_last = section == LAYERS - 1
    q_src = jnp.where(is_cross, 1, 0)

    win_copy = pltpu.make_async_copy(w_in, win, w_sem.at[0])
    wout_copy = pltpu.make_async_copy(w_out, wout, w_sem.at[1])
    win_copy.start()
    wout_copy.start()

    barrier = pltpu.get_barrier_semaphore()
    for step in range(1, segs):
        pl.semaphore_signal(
            barrier,
            inc=1,
            device_id={"segment": lax.rem(me + step, segs)},
            device_id_type=MESH,
        )
    pl.semaphore_wait(barrier, segs - 1)

    def remote(source, dest, send, recv, target):
        return pltpu.make_async_remote_copy(
            src_ref=source,
            dst_ref=dest,
            send_sem=send,
            recv_sem=recv,
            device_id={"segment": target},
            device_id_type=MESH,
        )

    def input_copy(kind, m, j):
        ref = src if kind == 0 else tgt
        target = 2 * kind * group + j
        return remote(
            ref.at[m],
            act.at[kind, m, me],
            in_send.at[kind, m, j],
            act_sem.at[kind, m, me],
            target,
        )

    def sends(kind, m, j):
        if kind == 1:
            return jnp.bool_(True)
        return jnp.logical_or(j == member, jnp.logical_and(section == 0, m > 0))

    def send_inputs(kind, m):
        ref = src if kind == 0 else tgt
        for j in range(group):
            target = 2 * kind * group + j

            @pl.when(jnp.logical_and(sends(kind, m, j), me != target))
            def _():
                input_copy(kind, m, j).start()

            @pl.when(me == target)
            def _():
                pltpu.make_async_copy(
                    ref.at[m], act.at[kind, m, me], act_sem.at[kind, m, me]
                ).start()

    def beside(g):
        return section * group + lax.rem(member + g, group)

    def side_copy(m, g):
        return remote(
            src.at[m],
            side.at[m - 1, g - 1],
            side_send.at[m - 1, g - 1],
            side_recv.at[m - 1, g - 1],
            beside(g),
        )

    def side_on(m, g):
        source = beside(group - g)
        return remote(
            side.at[m - 1, g - 1],
            act.at[0, m, source],
            on_send.at[m - 1, g - 1],
            act_sem.at[0, m, source],
            member,
        )

    def relay(c, g):
        return remote(
            act.at[0, 0, c],
            act.at[0, 0, c],
            r_send.at[g - 1, c],
            act_sem.at[0, 0, c],
            beside(g),
        )

    send_inputs(0, 0)

    @pl.when(section > 0)
    def _():
        for m in range(1, batches):
            for g in range(1, group):
                side_copy(m, g).start()

    @pl.when(section <= 2)
    def _():
        for m in range(batches):
            send_inputs(1, m)

    def act_wait(kind, m, c):
        pltpu.make_async_copy(
            act.at[kind, m, c], act.at[kind, m, c], act_sem.at[kind, m, c]
        ).wait()

    def pass_on():
        for c in range(segs):

            @pl.when(c % group == member)
            def _(c=c):
                act_wait(0, 0, c)
                for g in range(1, group):
                    relay(c, g).start()

    @pl.when(section == 0)
    def _():
        pass_on()
        for step in range(1, segs):
            pl.semaphore_signal(
                go,
                inc=1,
                device_id={"segment": lax.rem(me + step, segs)},
                device_id_type=MESH,
            )

    pl.semaphore_wait(go, jnp.where(section == 0, group - 1, group))
    for m in range(1, batches):
        send_inputs(0, m)

        @pl.when(section > 0)
        def _(m=m):
            for g in range(1, group):
                side_copy(m, g).wait_recv()
                side_on(m, g).start()

    @pl.when(section > 2)
    def _():
        for m in range(batches):
            send_inputs(1, m)

    def normalize(kind, m, gain_row):
        total = jnp.zeros((seq, cw), jnp.float32)
        for c in range(segs):
            v = act[kind, m, c].astype(jnp.float32)
            total = total + v * v
        mean = jnp.sum(total, axis=-1, keepdims=True) * (1.0 / width)
        scale = lax.rsqrt(mean + epsilon)
        for c in range(segs):
            v = act[kind, m, c].astype(jnp.float32)
            g = gain_row(c)
            nrm[kind, :, c * cw : (c + 1) * cw] = (v * scale * g).astype(jnp.bfloat16)

    def key_gain(c):
        cols = slice(c * cw, (c + 1) * cw)
        picked = jnp.where(is_cross, final_gain[:, cols], gains[0:1, cols])
        for p in (1, 3):
            picked = jnp.where(section == p, gains[p : p + 1, cols], picked)
        return picked

    def query_gain(c):
        return gains[2:3, c * cw : (c + 1) * cw]

    def part_copy(m, c, g):
        target = section * group + lax.rem(member + g, group)
        return remote(
            ps.at[m, c],
            pr.at[m, g - 1, c],
            p_send.at[m, g - 1, c],
            p_recv.at[m, g - 1, c],
            target,
        )

    def whole(m):
        return jnp.logical_and(section < LAYERS - 1, m > 0)

    def part_needed(m, c, g):
        goal = lax.rem(member + g, group)
        return jnp.logical_or(whole(m), lax.rem(c, group) == goal)

    def keeps(m, c):
        return jnp.logical_or(whole(m), lax.rem(c, group) == member)

    def next_copy(m, c):
        return remote(
            fw.at[m, c], act.at[0, m, c], f_send.at[m, c], act_sem.at[0, m, c], me + group
        )

    def out_copy(m, c):
        return remote(fw.at[m, c], out.at[m], f_send.at[m, c], o_recv.at[m], c)

    tile = min(512, hc)
    kv_tiles = 2 * hc // tile
    q_tiles = hc // tile

    def prepare(m):
        @pl.when(is_cross)
        def _():
            for c in range(segs):
                act_wait(1, m, c)
            normalize(1, m, query_gain)

        @pl.when(jnp.logical_and(section > 0, m == 0))
        def _():
            pass_on()

        for c in range(segs):

            @pl.when(jnp.logical_or(m > 0, c % group != member))
            def _(c=c):
                act_wait(0, m, c)

        normalize(0, m, key_gain)

        @pl.when(m == 0)
        def _():
            win_copy.wait()


    def project(t, carry):
        kind = jnp.where(t < q_tiles, q_src, 0)
        cols = pl.ds(pl.multiple_of(t * tile, tile), tile)
        qkv[:, cols] = jnp.dot(
            nrm[kind], win[:, cols], preferred_element_type=jnp.float32
        ).astype(jnp.bfloat16)
        return carry

    def attend(m):
        length = jnp.where(is_last, tgt_len[m], src_len[m])
        keys = lax.broadcasted_iota(jnp.int32, (2 * seq, seq), 1)
        rows = lax.broadcasted_iota(jnp.int32, (2 * seq, seq), 0)
        rows = jnp.where(rows >= seq, rows - seq, rows)
        bound = jnp.where(is_last, rows, seq)
        allowed = (keys < length) & (keys <= bound)
        lane = lax.broadcasted_iota(jnp.int32, (seq, 2 * HEAD), 1)
        low = lane < HEAD
        for h in range(hc // (2 * HEAD)):
            at = h * 2 * HEAD
            q2 = qkv[:, at : at + 2 * HEAD]
            k2 = qkv[:, hc + at : hc + at + 2 * HEAD]
            v2 = qkv[:, 2 * hc + at : 2 * hc + at + 2 * HEAD]
            zero = jnp.zeros_like(q2)
            both = jnp.concatenate(
                [jnp.where(low, q2, zero), jnp.where(low, zero, q2)], axis=0
            )
            scores = (
                lax.dot_general(
                    both,
                    k2,
                    (((1,), (1,)), ((), ())),
                    preferred_element_type=jnp.float32,
                )
                * score_scale
            )
            scores = jnp.where(allowed, scores, -1000000000.0)
            top = jnp.max(scores, axis=-1, keepdims=True)
            e = jnp.exp(scores - top)
            weights = (e / jnp.sum(e, axis=-1, keepdims=True)).astype(jnp.bfloat16)
            o = jnp.dot(weights, v2, preferred_element_type=jnp.float32)
            mix[:, at : at + 2 * HEAD] = jnp.where(low, o[:seq], o[seq:]).astype(
                jnp.bfloat16
            )

    def send_parts(m):
        @pl.when(m == 0)
        def _():
            wout_copy.wait()

        def emit(c, carry):
            cols = pl.ds(pl.multiple_of(c * cw, cw), cw)
            part = jnp.dot(mix[...], wout[:, cols], preferred_element_type=jnp.float32)
            own[c] = part
            ps[m, c] = part.astype(jnp.bfloat16)
            for g in range(1, group):

                @pl.when(part_needed(m, c, g))
                def _():
                    part_copy(m, c, g).start()

            return carry

        lax.fori_loop(0, segs, emit, 0, unroll=True)

    def combine(m, c):
        @pl.when(keeps(m, c))
        def _():
            total = own[c] + act[q_src, m, c].astype(jnp.float32)
            for g in range(1, group):
                part_copy(m, c, g).wait_recv()
                total = total + pr[m, g - 1, c].astype(jnp.float32)
            fw[m, c] = total.astype(jnp.bfloat16)

            @pl.when(section < LAYERS - 1)
            def _():
                next_copy(m, c).start()

            @pl.when(jnp.logical_and(is_last, me != c))
            def _():
                out_copy(m, c).start()

            @pl.when(jnp.logical_and(is_last, me == c))
            def _():
                pltpu.make_async_copy(fw.at[m, c], out.at[m], o_recv.at[m]).start()

    half = (q_tiles + kv_tiles) // 2
    stages = (
        prepare,
        lambda m: lax.fori_loop(0, half, project, 0, unroll=True),
        lambda m: lax.fori_loop(half, q_tiles + kv_tiles, project, 0, unroll=True),
        attend,
    )

    def batch_step(t, carry):
        m = t - 1

        @pl.when(t > 0)
        def _():
            send_parts(m)

        for c in range(segs):
            for i, stage in enumerate(stages):
                if c == segs // 2 + i * segs // 8:

                    @pl.when(t < batches)
                    def _(stage=stage):
                        stage(t)

            @pl.when(t > 0)
            def _(c=c):
                combine(m, c)

        return carry

    lax.fori_loop(0, batches + 1, batch_step, 0)

    def finish(m, carry):
        for kind in range(2):
            for j in range(group):

                @pl.when(jnp.logical_and(sends(kind, m, j), me != 2 * kind * group + j))
                def _():
                    input_copy(kind, m, j).wait_send()

        @pl.when(jnp.logical_and(section > 0, m > 0))
        def _():
            for g in range(1, group):
                side_copy(m, g).wait_send()
                side_on(m, g).wait_send()

        def drain(c, carry):
            for g in range(1, group):

                @pl.when(part_needed(m, c, g))
                def _():
                    part_copy(m, c, g).wait_send()

            @pl.when(jnp.logical_and(section < LAYERS - 1, keeps(m, c)))
            def _():
                next_copy(m, c).wait_send()

            @pl.when(jnp.logical_and(m == 0, lax.rem(c, group) == member))
            def _():
                for g in range(1, group):
                    relay(c, g).wait_send()

            @pl.when(jnp.logical_and(is_last, jnp.logical_and(keeps(m, c), me != c)))
            def _():
                out_copy(m, c).wait_send()

            return carry

        lax.fori_loop(0, segs, drain, 0)
        pltpu.make_async_copy(out.at[m], out.at[m], o_recv.at[m]).wait()
        return carry

    lax.fori_loop(0, batches, finish, 0)


def solution(mesh):
    segs = mesh.shape["segment"]

    def on_device(src, tgt, src_len, tgt_len, w_in, w_out, gains, final_gain):
        batches, seq, cw = src.shape
        group = segs // LAYERS
        w_in, w_out = w_in[0], w_out[0]
        width, qkv_cols = w_in.shape
        hc = w_out.shape[0]
        vmem = pl.BlockSpec(memory_space=pltpu.VMEM)
        smem = pl.BlockSpec(memory_space=pltpu.SMEM)
        anym = pl.BlockSpec(memory_space=pl.ANY)
        bf16 = jnp.bfloat16
        block = (segs, seq, cw)
        dma = pltpu.SemaphoreType.DMA
        return pl.pallas_call(
            functools.partial(kernel, segs),
            out_shape=jax.ShapeDtypeStruct(src.shape, src.dtype),
            in_specs=[smem, smem, vmem, vmem, anym, anym, vmem, vmem],
            out_specs=vmem,
            scratch_shapes=[
                pltpu.VMEM((width, qkv_cols), bf16),
                pltpu.VMEM((hc, width), bf16),
                pltpu.VMEM((2, batches) + block, bf16),
                pltpu.VMEM((2, seq, width), bf16),
                pltpu.VMEM((seq, qkv_cols), bf16),
                pltpu.VMEM((seq, hc), bf16),
                pltpu.VMEM(block, jnp.float32),
                pltpu.VMEM((batches,) + block, bf16),
                pltpu.VMEM((batches, group - 1) + block, bf16),
                pltpu.VMEM((batches,) + block, bf16),
                dma((2,)),
                dma((2, batches, segs)),
                dma((2, batches, group)),
                dma((batches, group - 1, segs)),
                dma((batches, group - 1, segs)),
                dma((batches, segs)),
                dma((batches,)),
                pltpu.SemaphoreType.REGULAR,
                pltpu.VMEM((batches - 1, group - 1, seq, cw), bf16),
                dma((batches - 1, group - 1)),
                dma((batches - 1, group - 1)),
                dma((batches - 1, group - 1)),
                dma((group - 1, segs)),
            ],
            compiler_params=pltpu.CompilerParams(
                collective_id=0,
                has_side_effects=True,
                vmem_limit_bytes=56 * 1024 * 1024,
            ),
        )(src_len, tgt_len, src, tgt, w_in, w_out, gains, final_gain[None])

    return jax.shard_map(
        on_device,
        mesh=mesh,
        in_specs=(
            P("dp", None, "segment"),
            P("dp", None, "segment"),
            P("dp"),
            P("dp"),
            P("segment", None, None),
            P("segment", None, None),
            P(),
            P(),
        ),
        out_specs=P("dp", None, "segment"),
        check_vma=False,
    )
```
